32 devices in a mesh: rep: 1 (over z), dp: 32 (over x, y, core).
Axes of the slice: x: 4, y: 4, z: 1, core: 2. Of those that a mesh axis runs over, the one named last changes fastest.
The devices are a block of a 4x4x8 slice.
Arguments:
- a: bfloat16 [32, 2, 4096, 1536], P(('rep', 'dp'))
- g: bfloat16 [32, 2, 4096, 4224], P(('rep', 'dp'))
Outputs:
- output: bfloat16 [2, 1536, 4224], P('rep')
All inputs are finite; a program needn't handle non-finite values.
Results may differ from the reference program's by a relative error of at most 0.012.
Values are sent between devices in bfloat16 or wider.
A program may use at most 768 MiB of HBM per device.

```python
import jax
import jax.numpy as jnp
from jax import lax

DEVICES = 32
MATRICES = 2
TOKENS = 4096
D = 1536
FF = 4224


def setup_inputs(seed: int = 0, part: int = 0) -> dict:
    ka, kg, ks = (jax.random.fold_in(k, part) for k in jax.random.split(jax.random.key(seed), 3))
    size = 2.0 ** jax.random.uniform(ks, (DEVICES, MATRICES, 1, 1), jnp.float32, -1.0, 1.0)
    a = jax.random.normal(ka, (DEVICES, MATRICES, TOKENS, D), jnp.float32)
    g = size * jax.random.normal(kg, (DEVICES, MATRICES, TOKENS, FF), jnp.float32) * (DEVICES * TOKENS) ** -0.5
    return {"a": a.astype(jnp.bfloat16), "g": g.astype(jnp.bfloat16)}


def reference(a, g):
    def take(so_far, one):
        return so_far + jnp.einsum("ntd,ntf->ndf", *one, preferred_element_type=jnp.float32), None

    return lax.scan(take, jnp.zeros((MATRICES, D, FF), jnp.float32), (a, g))[0].astype(jnp.bfloat16)
```

```python
import math

import jax
import jax.numpy as jnp
from jax import lax
from jax.experimental import pallas as pl
from jax.experimental.pallas import tpu as pltpu
from jax.sharding import PartitionSpec as P

MESH = pl.DeviceIdType.MESH
LANES = 128
F32 = jnp.float32
BF16 = jnp.bfloat16
OFFSETS = (0, 2, 4, 6, 8, 10, 12, 14, 16, 18)


def _reduce_kernel(side, mats, tiles, a, g, x, abuf, gbuf, acc, sd, s1, r, s2,
                   ssem, rsem, asem, gsem, credit):
    rows = x.shape[1]
    half = rows // 2
    blk = half // side
    sub = blk // side
    chunks = mats * tiles // 2
    mixed = tiles // 2 if tiles % 2 else -1
    nacc, ns1, nr, ns2 = acc.shape[0], s1.shape[0], r.shape[0], s2.shape[0]
    nss = ssem.shape[0]

    me = lax.axis_index("dp")
    core = lax.rem(me, 2)
    cy = lax.rem(me // 2, side)
    cx = me // (2 * side)
    p = jnp.where(core == 0, cx, cy)
    q = jnp.where(core == 0, cy, cx)

    def dev(i, j):
        return jnp.where(core == 0, (i * side + j) * 2, (j * side + i) * 2 + 1)

    def wrap(v):
        return lax.rem(v + 2 * side, side)

    first = (dev(wrap(p + 1), q), dev(wrap(p - 1), q))
    second = (dev(p, wrap(q + 1)), dev(p, wrap(q - 1)))
    partner = me + 1 - 2 * core
    mine = pl.multiple_of(core * half, half)
    other = pl.multiple_of((1 - core) * half, half)

    bar = pltpu.get_barrier_semaphore()
    for d in (*first, *second, partner):
        pl.semaphore_signal(bar, 1, device_id={"dp": d}, device_id_type=MESH)

    def copy(n, kind, src, dst, to):
        return pltpu.make_async_remote_copy(
            src_ref=src, dst_ref=dst, send_sem=ssem.at[lax.rem(n, nss), kind],
            recv_sem=rsem.at[n, kind], device_id={"dp": to}, device_id_type=MESH)

    def row(i, j=0):
        return pl.multiple_of(mine + wrap(i) * blk + wrap(j) * sub, sub)

    def pair(n, start, size):
        return x.at[pl.ds(2 * n, 2), pl.ds(start, size), :]

    def one(n, h, start, size):
        return x.at[2 * n + h, pl.ds(start, size), :]

    def c_half(n):
        return copy(n, 0, sd.at[lax.rem(n, 2)], pair(n, other, half), partner)

    def c_p1a(n, d):
        return copy(n, 1 + d, s1.at[lax.rem(n, ns1), d, pl.ds(0, 2 * blk), :],
                    one(n, d, other, 2 * blk), first[d])

    def c_p1b(n, d):
        return copy(n, 3 + d, s1.at[lax.rem(n, ns1), d, pl.ds(2 * blk, blk), :],
                    one(n, d, other + 2 * blk, blk), first[d])

    def c_p2a(n, d):
        return copy(n, 5 + d, s2.at[lax.rem(n, ns2), d, pl.ds(0, 2 * sub), :],
                    one(n, d, other + 3 * blk, 2 * sub), second[d])

    def c_p2b(n, d):
        return copy(n, 7 + d, s2.at[lax.rem(n, ns2), d, pl.ds(2 * sub, sub), :],
                    one(n, d, other + 3 * blk + 2 * sub, sub), second[d])

    def c_g2a(n, d):
        ref = pair(n, row(p, q), sub)
        return copy(n, 9 + d, ref, ref, second[d])

    def c_g2b(n, d):
        ref = one(n, d, row(p, q - 1 + 2 * d), sub)
        return copy(n, 11 + d, ref, ref, second[d])

    def c_g1a(n, d):
        ref = pair(n, row(p), blk)
        return copy(n, 13 + d, ref, ref, first[d])

    def c_g1b(n, d):
        ref = one(n, d, row(p - 1 + 2 * d), blk)
        return copy(n, 15 + d, ref, ref, first[d])

    def c_push(n):
        ref = pair(n, mine, half)
        return copy(n, 17, ref, ref, partner)

    def each(f, n, what):
        for d in range(2):
            getattr(f(n, d), what)()

    def got(n, h, start, size):
        return x[2 * n + h, pl.ds(start, size), :].astype(F32)

    def chip(n, h, i):
        at = pl.multiple_of(wrap(i) * blk, blk)
        return acc[lax.rem(n, nacc), h, pl.ds(at, blk), :] + got(n, h, row(i), blk)

    def line(n, h, j):
        at = pl.multiple_of(wrap(j) * sub, sub)
        return r[lax.rem(n, nr), h, pl.ds(at, sub), :]

    def stage1(n):
        c_half(n).wait_recv()
        sl = lax.rem(n, ns1)
        s1[sl, 0, pl.ds(0, blk), :] = chip(n, 1, p + 2).astype(BF16)
        s1[sl, 0, pl.ds(blk, blk), :] = chip(n, 0, p + 1).astype(BF16)
        s1[sl, 1, pl.ds(0, blk), :] = chip(n, 0, p + 2).astype(BF16)
        s1[sl, 1, pl.ds(blk, blk), :] = chip(n, 1, p - 1).astype(BF16)
        each(c_p1a, n, "start")

    def stage2(n):
        each(c_p1a, n, "wait_recv")
        c_half(n).wait_send()
        sl = lax.rem(n, ns1)
        s1[sl, 0, pl.ds(2 * blk, blk), :] = (chip(n, 1, p + 1) + got(n, 0, other, blk)).astype(BF16)
        s1[sl, 1, pl.ds(2 * blk, blk), :] = (chip(n, 0, p - 1) + got(n, 1, other, blk)).astype(BF16)
        each(c_p1b, n, "start")

    def stage3(n):
        each(c_p1b, n, "wait_recv")
        each(c_p1a, n, "wait_send")
        for h in range(2):
            r[lax.rem(n, nr), h] = (chip(n, h, p) + got(n, h, other + blk, blk)
                                    + got(n, 1 - h, other + 2 * blk, blk))
        sl = lax.rem(n, ns2)
        s2[sl, 0, pl.ds(0, sub), :] = line(n, 1, q + 2).astype(BF16)
        s2[sl, 0, pl.ds(sub, sub), :] = line(n, 0, q + 1).astype(BF16)
        s2[sl, 1, pl.ds(0, sub), :] = line(n, 0, q + 2).astype(BF16)
        s2[sl, 1, pl.ds(sub, sub), :] = line(n, 1, q - 1).astype(BF16)
        each(c_p2a, n, "start")

    def stage4(n):
        each(c_p2a, n, "wait_recv")
        each(c_p1b, n, "wait_send")
        sl = lax.rem(n, ns2)
        at = other + 3 * blk
        s2[sl, 0, pl.ds(2 * sub, sub), :] = (line(n, 1, q + 1) + got(n, 0, at, sub)).astype(BF16)
        s2[sl, 1, pl.ds(2 * sub, sub), :] = (line(n, 0, q - 1) + got(n, 1, at, sub)).astype(BF16)
        each(c_p2b, n, "start")

    def stage5(n):
        each(c_p2b, n, "wait_recv")
        each(c_p2a, n, "wait_send")
        at = other + 3 * blk
        for h in range(2):
            total = line(n, h, q) + got(n, h, at + sub, sub) + got(n, 1 - h, at + 2 * sub, sub)
            x[2 * n + h, pl.ds(row(p, q), sub), :] = total.astype(BF16)
        pl.semaphore_signal(credit, 1, device_id={"dp": partner}, device_id_type=MESH)
        each(c_g2a, n, "start")

    def stage6(n):
        each(c_g2a, n, "wait_recv")
        each(c_p2b, n, "wait_send")
        each(c_g2b, n, "start")

    def stage7(n):
        each(c_g2b, n, "wait_recv")
        each(c_g2a, n, "wait_send")
        each(c_g1a, n, "start")

    def stage8(n):
        each(c_g1a, n, "wait_recv")
        each(c_g2b, n, "wait_send")
        each(c_g1b, n, "start")

    def stage9(n):
        each(c_g1b, n, "wait_recv")
        each(c_g1a, n, "wait_send")
        pl.semaphore_wait(credit, 1)
        c_push(n).start()

    def stage10(n):
        c_push(n).wait_recv()
        c_push(n).wait_send()
        each(c_g1b, n, "wait_send")

    stages = (stage1, stage2, stage3, stage4, stage5, stage6, stage7, stage8, stage9, stage10)

    def a_load(m, part):
        cols = (other, mine)[part]
        view = (slice(None), pl.ds(cols, half))
        return pltpu.make_async_copy(a.at[(0, m) + view], abuf.at[(m,) + view], asem.at[m, part])

    def g_load(n, h):
        u = 2 * n + h
        c = pl.multiple_of(lax.rem(u, tiles) * LANES, LANES)
        sl = lax.rem(n, 2)
        return pltpu.make_async_copy(
            g.at[0, u // tiles, :, pl.ds(c, LANES)],
            gbuf.at[sl, :, pl.ds(h * LANES, LANES)], gsem.at[sl, h])

    def product(n, start, put):
        sl = lax.rem(n, 2)

        def dot(m, cols):
            return lax.dot_general(abuf[m, :, pl.ds(start, half)], gbuf[sl, :, cols],
                                   (((0,), (0,)), ((), ())), preferred_element_type=F32)

        @pl.when(n != mixed)
        def _():
            out = dot((2 * n) // tiles, slice(None))
            for h in range(2):
                put(h, out[:, h * LANES:(h + 1) * LANES])

        if mixed >= 0:
            @pl.when(n == mixed)
            def _():
                for h in range(2):
                    put(h, dot((2 * n + h) // tiles, slice(h * LANES, (h + 1) * LANES)))

    def run_stages(step, parity):
        for k in reversed(range(len(stages))):
            if (OFFSETS[k] + 1) % 2 != parity:
                continue
            n = step - (OFFSETS[k] + 1 - parity) // 2

            @pl.when(jnp.logical_and(n >= 0, n < chunks))
            def _(k=k, n=n):
                stages[k](n)

    a_load(0, 0).start()
    for h in range(2):
        g_load(0, h).start()
    a_load(0, 1).start()
    pl.semaphore_wait(bar, 5)

    def step(t, _):
        @pl.when(t < chunks)
        def _():
            @pl.when(t + 1 < chunks)
            def _():
                for h in range(2):
                    g_load(t + 1, h).start()
            for h in range(2):
                g_load(t, h).wait()
            for m in range(mats):
                @pl.when(t == m * tiles // 2)
                def _(m=m):
                    a_load(m, 0).wait()

            def put(h, v):
                sd[lax.rem(t, 2), h] = v.astype(BF16)

            product(t, other, put)
            c_half(t).start()

        run_stages(t, 0)

        @pl.when(t < chunks)
        def _():
            for m in range(mats):
                @pl.when(t == m * tiles // 2)
                def _(m=m):
                    a_load(m, 1).wait()

            def put(h, v):
                acc[lax.rem(t, nacc), h] = v

            product(t, mine, put)
            for m in range(1, mats):
                @pl.when(t == (m - 1) * tiles // 2)
                def _(m=m):
                    for part in range(2):
                        a_load(m, part).start()

        run_stages(t, 1)
        return 0

    lax.fori_loop(0, chunks + (max(OFFSETS) + 1) // 2, step, 0)


def _write_kernel(x, out, sem):
    tiles = x.shape[0] // out.shape[0]

    def moves():
        for u in range(x.shape[0]):
            yield pltpu.make_async_copy(
                x.at[u], out.at[u // tiles, :, pl.ds(u % tiles * LANES, LANES)], sem.at[u])

    for move in moves():
        move.start()
    for move in moves():
        move.wait()


def solution(mesh):
    cores = 2
    side = math.isqrt(mesh.shape["dp"] // cores)

    def body(a, g):
        _, mats, tokens, rows = a.shape
        tiles = g.shape[-1] // LANES
        half = rows // 2
        blk = half // side
        sub = blk // side
        chunks = mats * tiles // 2
        keep = OFFSETS[2] // 2 + 2
        x = pl.pallas_call(
            lambda *refs: _reduce_kernel(side, mats, tiles, *refs),
            out_shape=pltpu.VMEM((mats * tiles, rows, LANES), BF16),
            in_specs=[pl.BlockSpec(memory_space=pl.ANY)] * 2,
            out_specs=pl.BlockSpec(memory_space=pltpu.VMEM),
            scratch_shapes=[
                pltpu.VMEM((mats, tokens, rows), BF16),
                pltpu.VMEM((2, tokens, 2 * LANES), BF16),
                pltpu.VMEM((keep, 2, half, LANES), F32),
                pltpu.VMEM((2, 2, half, LANES), BF16),
                pltpu.VMEM((4, 2, 3 * blk, LANES), BF16),
                pltpu.VMEM((4, 2, blk, LANES), F32),
                pltpu.VMEM((4, 2, 3 * sub, LANES), BF16),
                pltpu.SemaphoreType.DMA((4, 18)),
                pltpu.SemaphoreType.DMA((chunks, 18)),
                pltpu.SemaphoreType.DMA((mats, 2)),
                pltpu.SemaphoreType.DMA((2, 2)),
                pltpu.SemaphoreType.REGULAR,
            ],
            compiler_params=pltpu.CompilerParams(
                collective_id=0, has_side_effects=True, vmem_limit_bytes=39 * 2**20),
            name="reduce",
        )(a, g)
        return pl.pallas_call(
            _write_kernel,
            out_shape=jax.ShapeDtypeStruct((mats, rows, tiles * LANES), BF16),
            in_specs=[pl.BlockSpec(memory_space=pltpu.VMEM)],
            out_specs=pl.BlockSpec(memory_space=pl.ANY),
            scratch_shapes=[pltpu.SemaphoreType.DMA((mats * tiles,))],
            compiler_params=pltpu.CompilerParams(vmem_limit_bytes=2**20),
            name="write",
        )(x)

    spec = P(("rep", "dp"))
    return jax.shard_map(body, mesh=mesh, in_specs=(spec, spec), out_specs=P("rep"), check_vma=False)
```

```python
import math

import jax
import jax.numpy as jnp
from jax import lax
from jax.experimental import pallas as pl
from jax.experimental.pallas import tpu as pltpu
from jax.sharding import PartitionSpec as P

MESH = pl.DeviceIdType.MESH
HALF, P1A, P1B, P2A, P2B, G2A, G2B, G1A, G1B, PUSH = range(10)
SENT = (0, 1, 1, 2, 2, 3, 3, 3, 3, 3)
LANES = 128
F32 = jnp.float32
BF16 = jnp.bfloat16
OFFSETS = (1, 3, 4, 5, 6, 7, 8, 10, 12, 13)
ORDER = (5, 6, 4, 3, 2, 1, 7, 8, 9, 10)


def _reduce_kernel(side, mats, tiles, a, g, x, abuf, gbuf, acc, sd, s1, r, s2,
                   ssem, rsem, asem, gsem, credit):
    rows = x.shape[1]
    half = rows // 2
    blk = half // side
    sub = blk // side
    chunks = mats * tiles // 2
    mixed = tiles // 2 if tiles % 2 else -1
    nacc = acc.shape[0]

    def slot(n):
        return n & 7

    def acc_slot(n):
        return n - nacc * (n * (1024 // nacc + 1) // 1024)

    me = lax.axis_index("dp")
    core = lax.rem(me, 2)
    cy = lax.rem(me // 2, side)
    cx = me // (2 * side)
    p = jnp.where(core == 0, cx, cy)
    q = jnp.where(core == 0, cy, cx)

    def dev(i, j):
        return jnp.where(core == 0, (i * side + j) * 2, (j * side + i) * 2 + 1)

    def wrap(v):
        return lax.rem(v + 2 * side, side)

    first = (dev(wrap(p + 1), q), dev(wrap(p - 1), q))
    second = (dev(p, wrap(q + 1)), dev(p, wrap(q - 1)))
    partner = me + 1 - 2 * core
    mine = pl.multiple_of(core * half, half)
    other = pl.multiple_of((1 - core) * half, half)

    bar = pltpu.get_barrier_semaphore()
    for d in (*first, *second, partner):
        pl.semaphore_signal(bar, 1, device_id={"dp": d}, device_id_type=MESH)

    def copy(n, kind, src, dst, to):
        return pltpu.make_async_remote_copy(
            src_ref=src, dst_ref=dst, send_sem=ssem.at[slot(n), SENT[kind]],
            recv_sem=rsem.at[n, kind], device_id={"dp": to}, device_id_type=MESH)

    def landed(n, kind, size):
        ref = pair(n, 0, size)
        pltpu.make_async_copy(ref, ref, rsem.at[n, kind]).wait()

    def left(n, group, size):
        ref = pair(n, 0, size)
        pltpu.make_async_copy(ref, ref, ssem.at[slot(n), group]).wait()

    def row(i, j=0):
        return pl.multiple_of(mine + wrap(i) * blk + wrap(j) * sub, sub)

    first_at = {i: pl.multiple_of(wrap(p + i) * blk, blk) for i in (-1, 0, 1, 2)}
    second_at = {j: pl.multiple_of(wrap(q + j) * sub, sub) for j in (-1, 0, 1, 2)}
    home = {(i, j): row(p + i, q + j) for i, j in ((0, 0), (0, -1), (0, 1))}
    row_at = {i: row(p + i) for i in (-1, 0, 1, 2)}

    def pair(n, start, size):
        return x.at[pl.ds(2 * n, 2), pl.ds(start, size), :]

    def one(n, h, start, size):
        return x.at[2 * n + h, pl.ds(start, size), :]

    def c_half(n):
        return copy(n, HALF, sd.at[(n & 1)], pair(n, other, half), partner)

    def c_p1a(n, d):
        return copy(n, P1A, s1.at[n & 3, d, pl.ds(0, 2 * blk), :],
                    one(n, d, other, 2 * blk), first[d])

    def c_p1b(n, d):
        return copy(n, P1B, s1.at[n & 3, d, pl.ds(2 * blk, blk), :],
                    one(n, d, other + 2 * blk, blk), first[d])

    def c_p2a(n, d):
        return copy(n, P2A, s2.at[slot(n), d, pl.ds(0, 2 * sub), :],
                    one(n, d, other + 3 * blk, 2 * sub), second[d])

    def c_p2b(n, d):
        return copy(n, P2B, s2.at[slot(n), d, pl.ds(2 * sub, sub), :],
                    one(n, d, other + 3 * blk + 2 * sub, sub), second[d])

    def c_g2a(n, d):
        ref = pair(n, home[0, 0], sub)
        return copy(n, G2A, ref, ref, second[d])

    def c_g2b(n, d):
        ref = one(n, d, home[0, 2 * d - 1], sub)
        return copy(n, G2B, ref, ref, second[d])

    def c_g1a(n, d):
        ref = pair(n, row_at[0], blk)
        return copy(n, G1A, ref, ref, first[d])

    def c_g1b(n, d):
        ref = one(n, d, row_at[2 * d - 1], blk)
        return copy(n, G1B, ref, ref, first[d])

    def c_push(n):
        ref = pair(n, mine, half)
        return copy(n, PUSH, ref, ref, partner)

    def each(f, n, what):
        for d in range(2):
            getattr(f(n, d), what)()

    def got(n, h, start, size):
        return x[2 * n + h, pl.ds(start, size), :].astype(F32)

    def chip(n, h, i):
        return acc[acc_slot(n), h, pl.ds(first_at[i], blk), :] + got(n, h, row_at[i], blk)

    def line(n, h, j):
        return r[n & 3, h, pl.ds(second_at[j], sub), :]

    def stage1(n):
        c_half(n).wait_recv()
        c_half(n).wait_send()
        sl = n & 3
        s1[sl, 0, pl.ds(0, blk), :] = chip(n, 1, 2).astype(BF16)
        s1[sl, 0, pl.ds(blk, blk), :] = chip(n, 0, 1).astype(BF16)
        s1[sl, 1, pl.ds(0, blk), :] = chip(n, 0, 2).astype(BF16)
        s1[sl, 1, pl.ds(blk, blk), :] = chip(n, 1, -1).astype(BF16)
        each(c_p1a, n, "start")

    def stage2(n):
        landed(n, P1A, 2 * blk)
        sl = n & 3
        s1[sl, 0, pl.ds(2 * blk, blk), :] = (chip(n, 1, 1) + got(n, 0, other, blk)).astype(BF16)
        s1[sl, 1, pl.ds(2 * blk, blk), :] = (chip(n, 0, -1) + got(n, 1, other, blk)).astype(BF16)
        each(c_p1b, n, "start")

    def stage3(n):
        landed(n, P1B, blk)
        for h in range(2):
            r[(n & 3), h] = (chip(n, h, 0) + got(n, h, other + blk, blk)
                                    + got(n, 1 - h, other + 2 * blk, blk))
        sl = slot(n)
        s2[sl, 0, pl.ds(0, sub), :] = line(n, 1, 2).astype(BF16)
        s2[sl, 0, pl.ds(sub, sub), :] = line(n, 0, 1).astype(BF16)
        s2[sl, 1, pl.ds(0, sub), :] = line(n, 0, 2).astype(BF16)
        s2[sl, 1, pl.ds(sub, sub), :] = line(n, 1, -1).astype(BF16)
        each(c_p2a, n, "start")

    def stage4(n):
        landed(n, P2A, 2 * sub)
        left(n, 1, 3 * blk)
        sl = slot(n)
        at = other + 3 * blk
        s2[sl, 0, pl.ds(2 * sub, sub), :] = (line(n, 1, 1) + got(n, 0, at, sub)).astype(BF16)
        s2[sl, 1, pl.ds(2 * sub, sub), :] = (line(n, 0, -1) + got(n, 1, at, sub)).astype(BF16)
        each(c_p2b, n, "start")

    def stage5(n):
        landed(n, P2B, sub)
        at = other + 3 * blk
        for h in range(2):
            total = line(n, h, 0) + got(n, h, at + sub, sub) + got(n, 1 - h, at + 2 * sub, sub)
            x[2 * n + h, pl.ds(home[0, 0], sub), :] = total.astype(BF16)
        pl.semaphore_signal(credit, 1, device_id={"dp": partner}, device_id_type=MESH)
        each(c_g2a, n, "start")

    def stage6(n):
        landed(n, G2A, 2 * sub)
        left(n, 2, 3 * sub)
        each(c_g2b, n, "start")

    def stage7(n):
        landed(n, G2B, sub)
        each(c_g1a, n, "start")

    def stage8(n):
        landed(n, G1A, 2 * blk)
        each(c_g1b, n, "start")

    def stage9(n):
        landed(n, G1B, blk)
        pl.semaphore_wait(credit, 1)
        c_push(n).start()

    def stage10(n):
        c_push(n).wait_recv()
        left(n, 3, half + 3 * blk + 3 * sub)

    stages = (stage1, stage2, stage3, stage4, stage5, stage6, stage7, stage8, stage9, stage10)

    def a_load(m, part):
        cols = (other, mine)[part]
        view = (slice(None), pl.ds(cols, half))
        return pltpu.make_async_copy(a.at[(0, m) + view], abuf.at[(m,) + view], asem.at[m, part])

    def g_load(n, h):
        u = 2 * n + h
        c = pl.multiple_of(lax.rem(u, tiles) * LANES, LANES)
        sl = (n & 1)
        return pltpu.make_async_copy(
            g.at[0, u // tiles, :, pl.ds(c, LANES)],
            gbuf.at[sl, :, pl.ds(h * LANES, LANES)], gsem.at[sl, h])

    def product(n, same):
        sl = (n & 1)

        def dot(start, h, cols):
            return lax.dot_general(abuf[(2 * n + h) // tiles, :, pl.ds(start, half)], gbuf[sl, :, cols],
                                   (((0,), (0,)), ((), ())), preferred_element_type=F32)

        def halves(start):
            if same:
                both = dot(start, 0, slice(None))
                return [both[:, h * LANES:(h + 1) * LANES] for h in range(2)]
            return [lax.dot_general(
                gbuf[sl, :, h * LANES:(h + 1) * LANES], abuf[(2 * n + h) // tiles, :, pl.ds(start, half)],
                (((0,), (0,)), ((), ())), preferred_element_type=F32).T for h in range(2)]

        for h, v in enumerate(halves(other)):
            sd[sl, h] = v.astype(BF16)
        for h, v in enumerate(halves(mine)):
            acc[acc_slot(n), h] = v
        c_half(n).start()

    def run_stages(t):
        for k in ORDER:
            n = t - OFFSETS[k - 1]

            @pl.when(jnp.logical_and(n >= 0, n < chunks))
            def _(k=k, n=n):
                stages[k - 1](n)

    a_load(0, 0).start()
    for h in range(2):
        g_load(0, h).start()
    a_load(0, 1).start()
    pl.semaphore_wait(bar, 5)

    def step(t, _):
        @pl.when(t < chunks)
        def _():
            @pl.when(t + 1 < chunks)
            def _():
                for h in range(2):
                    g_load(t + 1, h).start()
            for m in range(mats):
                @pl.when(t == m * tiles // 2)
                def _(m=m):
                    for part in range(2):
                        a_load(m, part).wait()
            for h in range(2):
                g_load(t, h).wait()
            for m in range(1, mats):
                @pl.when(t == (m - 1) * tiles // 2 + 1)
                def _(m=m):
                    for part in range(2):
                        a_load(m, part).start()

        @pl.when(jnp.logical_and(t < chunks, t != mixed))
        def _():
            product(t, True)

        if mixed >= 0:
            @pl.when(t == mixed)
            def _():
                product(t, False)

        run_stages(t)
        return 0

    lax.fori_loop(0, chunks + max(OFFSETS), step, 0)


def _write_kernel(x, out, sem):
    tiles = x.shape[0] // out.shape[0]

    def moves():
        for u in range(x.shape[0]):
            yield pltpu.make_async_copy(
                x.at[u], out.at[u // tiles, :, pl.ds(u % tiles * LANES, LANES)], sem.at[u])

    for move in moves():
        move.start()
    for move in moves():
        move.wait()


def solution(mesh):
    cores = 2
    side = math.isqrt(mesh.shape["dp"] // cores)

    def body(a, g):
        _, mats, tokens, rows = a.shape
        tiles = g.shape[-1] // LANES
        half = rows // 2
        blk = half // side
        sub = blk // side
        chunks = mats * tiles // 2
        keep = OFFSETS[2] + 1
        x = pl.pallas_call(
            lambda *refs: _reduce_kernel(side, mats, tiles, *refs),
            out_shape=pltpu.VMEM((mats * tiles, rows, LANES), BF16),
            in_specs=[pl.BlockSpec(memory_space=pl.ANY)] * 2,
            out_specs=pl.BlockSpec(memory_space=pltpu.VMEM),
            scratch_shapes=[
                pltpu.VMEM((mats, tokens, rows), BF16),
                pltpu.VMEM((2, tokens, 2 * LANES), BF16),
                pltpu.VMEM((keep, 2, half, LANES), F32),
                pltpu.VMEM((2, 2, half, LANES), BF16),
                pltpu.VMEM((4, 2, 3 * blk, LANES), BF16),
                pltpu.VMEM((4, 2, blk, LANES), F32),
                pltpu.VMEM((8, 2, 3 * sub, LANES), BF16),
                pltpu.SemaphoreType.DMA((8, 4)),
                pltpu.SemaphoreType.DMA((chunks, 10)),
                pltpu.SemaphoreType.DMA((mats, 2)),
                pltpu.SemaphoreType.DMA((2, 2)),
                pltpu.SemaphoreType.REGULAR,
            ],
            compiler_params=pltpu.CompilerParams(
                collective_id=0, has_side_effects=True, vmem_limit_bytes=39 * 2**20),
            name="reduce",
        )(a, g)
        return pl.pallas_call(
            _write_kernel,
            out_shape=jax.ShapeDtypeStruct((mats, rows, tiles * LANES), BF16),
            in_specs=[pl.BlockSpec(memory_space=pltpu.VMEM)],
            out_specs=pl.BlockSpec(memory_space=pl.ANY),
            scratch_shapes=[pltpu.SemaphoreType.DMA((mats * tiles,))],
            compiler_params=pltpu.CompilerParams(vmem_limit_bytes=2**20),
            name="write",
        )(x)

    spec = P(("rep", "dp"))
    return jax.shard_map(body, mesh=mesh, in_specs=(spec, spec), out_specs=P("rep"), check_vma=False)
```

```python
import math

import jax
import jax.numpy as jnp
from jax import lax
from jax.experimental import pallas as pl
from jax.experimental.pallas import tpu as pltpu
from jax.sharding import PartitionSpec as P

MESH = pl.DeviceIdType.MESH
HALF, P1A, P1B, P2A, P2B, G2A, G2B, G1A, G1B, PUSH = range(10)
SENT = (0, 1, 1, 2, 2, 3, 3, 3, 3, 3)
LANES = 128
F32 = jnp.float32
BF16 = jnp.bfloat16
OFFSETS = (1, 3, 4, 5, 6, 7, 8, 10, 12, 13)
ORDER = (5, 6, 4, 3, 2, 1, 7, 8, 9, 10)


def _reduce_kernel(side, mats, tiles, a, g, x, abuf, gbuf, acc, sd, s1, r, s2,
                   ssem, rsem, asem, gsem, credit):
    rows = x.shape[1]
    half = rows // 2
    blk = half // side
    sub = blk // side
    chunks = mats * tiles // 2
    mixed = tiles // 2 if tiles % 2 else -1
    nacc = acc.shape[0]

    def slot(n):
        return n & 7

    def acc_slot(n):
        return n - nacc * (n * (1024 // nacc + 1) // 1024)

    me = lax.axis_index("dp")
    core = lax.rem(me, 2)
    cy = lax.rem(me // 2, side)
    cx = me // (2 * side)
    p = jnp.where(core == 0, cx, cy)
    q = jnp.where(core == 0, cy, cx)

    def dev(i, j):
        return jnp.where(core == 0, (i * side + j) * 2, (j * side + i) * 2 + 1)

    def wrap(v):
        return lax.rem(v + 2 * side, side)

    first = (dev(wrap(p + 1), q), dev(wrap(p - 1), q))
    second = (dev(p, wrap(q + 1)), dev(p, wrap(q - 1)))
    partner = me + 1 - 2 * core
    mine = pl.multiple_of(core * half, half)
    other = pl.multiple_of((1 - core) * half, half)

    bar = pltpu.get_barrier_semaphore()
    for d in (*first, *second, partner):
        pl.semaphore_signal(bar, 1, device_id={"dp": d}, device_id_type=MESH)

    def copy(n, kind, src, dst, to):
        return pltpu.make_async_remote_copy(
            src_ref=src, dst_ref=dst, send_sem=ssem.at[slot(n), SENT[kind]],
            recv_sem=rsem.at[n, kind], device_id={"dp": to}, device_id_type=MESH)

    def landed(n, kind, size):
        ref = pair(n, 0, size)
        pltpu.make_async_copy(ref, ref, rsem.at[n, kind]).wait()

    def left(n, group, size):
        ref = pair(n, 0, size)
        pltpu.make_async_copy(ref, ref, ssem.at[slot(n), group]).wait()

    def row(i, j=0):
        return pl.multiple_of(mine + wrap(i) * blk + wrap(j) * sub, sub)

    first_at = {i: pl.multiple_of(wrap(p + i) * blk, blk) for i in (-1, 0, 1, 2)}
    second_at = {j: pl.multiple_of(wrap(q + j) * sub, sub) for j in (-1, 0, 1, 2)}
    home = {(i, j): row(p + i, q + j) for i, j in ((0, 0), (0, -1), (0, 1))}
    row_at = {i: row(p + i) for i in (-1, 0, 1, 2)}

    def pair(n, start, size):
        return x.at[pl.ds(2 * n, 2), pl.ds(start, size), :]

    def one(n, h, start, size):
        return x.at[2 * n + h, pl.ds(start, size), :]

    def c_half(n):
        return copy(n, HALF, sd.at[(n & 1)], pair(n, other, half), partner)

    def c_p1a(n, d):
        return copy(n, P1A, s1.at[n & 3, d, pl.ds(0, 2 * blk), :],
                    one(n, d, other, 2 * blk), first[d])

    def c_p1b(n, d):
        return copy(n, P1B, s1.at[n & 3, d, pl.ds(2 * blk, blk), :],
                    one(n, d, other + 2 * blk, blk), first[d])

    def c_p2a(n, d):
        return copy(n, P2A, s2.at[slot(n), d, pl.ds(0, 2 * sub), :],
                    one(n, d, other + 3 * blk, 2 * sub), second[d])

    def c_p2b(n, d):
        return copy(n, P2B, s2.at[slot(n), d, pl.ds(2 * sub, sub), :],
                    one(n, d, other + 3 * blk + 2 * sub, sub), second[d])

    def c_g2a(n, d):
        ref = pair(n, home[0, 0], sub)
        return copy(n, G2A, ref, ref, second[d])

    def c_g2b(n, d):
        ref = one(n, d, home[0, 2 * d - 1], sub)
        return copy(n, G2B, ref, ref, second[d])

    def c_g1a(n, d):
        ref = pair(n, row_at[0], blk)
        return copy(n, G1A, ref, ref, first[d])

    def c_g1b(n, d):
        ref = one(n, d, row_at[2 * d - 1], blk)
        return copy(n, G1B, ref, ref, first[d])

    def c_push(n):
        ref = pair(n, mine, half)
        return copy(n, PUSH, ref, ref, partner)

    def each(f, n, what):
        for d in range(2):
            getattr(f(n, d), what)()

    def got(n, h, start, size):
        return x[2 * n + h, pl.ds(start, size), :].astype(F32)

    def chip(n, h, i):
        return acc[acc_slot(n), h, pl.ds(first_at[i], blk), :] + got(n, h, row_at[i], blk)

    def line(n, h, j):
        return r[n & 3, h, pl.ds(second_at[j], sub), :]

    def stage1(n):
        c_half(n).wait_recv()
        c_half(n).wait_send()
        sl = n & 3
        s1[sl, 0, pl.ds(0, blk), :] = chip(n, 1, 2).astype(BF16)
        s1[sl, 0, pl.ds(blk, blk), :] = chip(n, 0, 1).astype(BF16)
        s1[sl, 1, pl.ds(0, blk), :] = chip(n, 0, 2).astype(BF16)
        s1[sl, 1, pl.ds(blk, blk), :] = chip(n, 1, -1).astype(BF16)
        each(c_p1a, n, "start")

    def stage2(n):
        landed(n, P1A, 2 * blk)
        sl = n & 3
        s1[sl, 0, pl.ds(2 * blk, blk), :] = (chip(n, 1, 1) + got(n, 0, other, blk)).astype(BF16)
        s1[sl, 1, pl.ds(2 * blk, blk), :] = (chip(n, 0, -1) + got(n, 1, other, blk)).astype(BF16)
        each(c_p1b, n, "start")

    def stage3(n):
        landed(n, P1B, blk)
        left(n, 1, 3 * blk)
        for h in range(2):
            r[(n & 3), h] = (chip(n, h, 0) + got(n, h, other + blk, blk)
                                    + got(n, 1 - h, other + 2 * blk, blk))
        sl = slot(n)
        s2[sl, 0, pl.ds(0, sub), :] = line(n, 1, 2).astype(BF16)
        s2[sl, 0, pl.ds(sub, sub), :] = line(n, 0, 1).astype(BF16)
        s2[sl, 1, pl.ds(0, sub), :] = line(n, 0, 2).astype(BF16)
        s2[sl, 1, pl.ds(sub, sub), :] = line(n, 1, -1).astype(BF16)
        each(c_p2a, n, "start")

    def stage4(n):
        landed(n, P2A, 2 * sub)
        sl = slot(n)
        at = other + 3 * blk
        s2[sl, 0, pl.ds(2 * sub, sub), :] = (line(n, 1, 1) + got(n, 0, at, sub)).astype(BF16)
        s2[sl, 1, pl.ds(2 * sub, sub), :] = (line(n, 0, -1) + got(n, 1, at, sub)).astype(BF16)
        each(c_p2b, n, "start")

    def stage5(n):
        landed(n, P2B, sub)
        at = other + 3 * blk
        for h in range(2):
            total = line(n, h, 0) + got(n, h, at + sub, sub) + got(n, 1 - h, at + 2 * sub, sub)
            x[2 * n + h, pl.ds(home[0, 0], sub), :] = total.astype(BF16)
        pl.semaphore_signal(credit, 1, device_id={"dp": partner}, device_id_type=MESH)
        each(c_g2a, n, "start")

    def stage6(n):
        landed(n, G2A, 2 * sub)
        left(n, 2, 3 * sub)
        each(c_g2b, n, "start")

    def stage7(n):
        landed(n, G2B, sub)
        each(c_g1a, n, "start")

    def stage8(n):
        landed(n, G1A, 2 * blk)
        each(c_g1b, n, "start")

    def stage9(n):
        landed(n, G1B, blk)
        pl.semaphore_wait(credit, 1)
        c_push(n).start()

    def stage10(n):
        c_push(n).wait_recv()
        left(n, 3, half + 3 * blk + 3 * sub)

    stages = (stage1, stage2, stage3, stage4, stage5, stage6, stage7, stage8, stage9, stage10)

    def a_load(m, part):
        cols = (other, mine)[part]
        view = (slice(None), pl.ds(cols, half))
        return pltpu.make_async_copy(a.at[(0, m) + view], abuf.at[(m,) + view], asem.at[m, part])

    def g_load(n, h):
        u = 2 * n + h
        c = pl.multiple_of(lax.rem(u, tiles) * LANES, LANES)
        sl = (n & 1)
        return pltpu.make_async_copy(
            g.at[0, u // tiles, :, pl.ds(c, LANES)],
            gbuf.at[sl, :, pl.ds(h * LANES, LANES)], gsem.at[sl, h])

    def product(n, same):
        sl = (n & 1)

        def dot(start, h, cols):
            return lax.dot_general(abuf[(2 * n + h) // tiles, :, pl.ds(start, half)], gbuf[sl, :, cols],
                                   (((0,), (0,)), ((), ())), preferred_element_type=F32)

        def halves(start):
            if same:
                both = dot(start, 0, slice(None))
                return [both[:, h * LANES:(h + 1) * LANES] for h in range(2)]
            return [lax.dot_general(
                gbuf[sl, :, h * LANES:(h + 1) * LANES], abuf[(2 * n + h) // tiles, :, pl.ds(start, half)],
                (((0,), (0,)), ((), ())), preferred_element_type=F32).T for h in range(2)]

        for h, v in enumerate(halves(other)):
            sd[sl, h] = v.astype(BF16)
        for h, v in enumerate(halves(mine)):
            acc[acc_slot(n), h] = v
        c_half(n).start()

    def run_stages(t):
        for k in ORDER:
            n = t - OFFSETS[k - 1]

            @pl.when(n >= 0)
            def _(k=k, n=n):
                stages[k - 1](n)

    a_load(0, 0).start()
    for h in range(2):
        g_load(0, h).start()
    a_load(0, 1).start()
    pl.semaphore_wait(bar, 5)

    def step(t, _):
        @pl.when(t + 1 < chunks)
        def _():
            for h in range(2):
                g_load(t + 1, h).start()
        for m in range(mats):
            @pl.when(t == m * tiles // 2)
            def _(m=m):
                for part in range(2):
                    a_load(m, part).wait()
        for h in range(2):
            g_load(t, h).wait()
        for m in range(1, mats):
            @pl.when(t == (m - 1) * tiles // 2 + 1)
            def _(m=m):
                for part in range(2):
                    a_load(m, part).start()

        @pl.when(t != mixed)
        def _():
            product(t, True)

        if mixed >= 0:
            @pl.when(t == mixed)
            def _():
                product(t, False)

        run_stages(t)
        return 0

    lax.fori_loop(0, chunks, step, 0)

    todo = {n: sum(n + o < chunks for o in OFFSETS) for n in range(chunks)}
    while any(k < len(stages) for k in todo.values()):
        for n in sorted((n for n in todo if todo[n] < len(stages)), key=lambda n: ORDER.index(todo[n] + 1)):
            stages[todo[n]](n)
            todo[n] += 1


def _write_kernel(x, out, sem):
    tiles = x.shape[0] // out.shape[0]

    def moves():
        for u in range(x.shape[0]):
            yield pltpu.make_async_copy(
                x.at[u], out.at[u // tiles, :, pl.ds(u % tiles * LANES, LANES)], sem.at[u])

    for move in moves():
        move.start()
    for move in moves():
        move.wait()


def solution(mesh):
    cores = 2
    side = math.isqrt(mesh.shape["dp"] // cores)

    def body(a, g):
        _, mats, tokens, rows = a.shape
        tiles = g.shape[-1] // LANES
        half = rows // 2
        blk = half // side
        sub = blk // side
        chunks = mats * tiles // 2
        keep = OFFSETS[2] + 1
        x = pl.pallas_call(
            lambda *refs: _reduce_kernel(side, mats, tiles, *refs),
            out_shape=pltpu.VMEM((mats * tiles, rows, LANES), BF16),
            in_specs=[pl.BlockSpec(memory_space=pl.ANY)] * 2,
            out_specs=pl.BlockSpec(memory_space=pltpu.VMEM),
            scratch_shapes=[
                pltpu.VMEM((mats, tokens, rows), BF16),
                pltpu.VMEM((2, tokens, 2 * LANES), BF16),
                pltpu.VMEM((keep, 2, half, LANES), F32),
                pltpu.VMEM((2, 2, half, LANES), BF16),
                pltpu.VMEM((4, 2, 3 * blk, LANES), BF16),
                pltpu.VMEM((4, 2, blk, LANES), F32),
                pltpu.VMEM((8, 2, 3 * sub, LANES), BF16),
                pltpu.SemaphoreType.DMA((8, 4)),
                pltpu.SemaphoreType.DMA((chunks, 10)),
                pltpu.SemaphoreType.DMA((mats, 2)),
                pltpu.SemaphoreType.DMA((2, 2)),
                pltpu.SemaphoreType.REGULAR,
            ],
            compiler_params=pltpu.CompilerParams(
                collective_id=0, has_side_effects=True, vmem_limit_bytes=39 * 2**20),
            name="reduce",
        )(a, g)
        return pl.pallas_call(
            _write_kernel,
            out_shape=jax.ShapeDtypeStruct((mats, rows, tiles * LANES), BF16),
            in_specs=[pl.BlockSpec(memory_space=pltpu.VMEM)],
            out_specs=pl.BlockSpec(memory_space=pl.ANY),
            scratch_shapes=[pltpu.SemaphoreType.DMA((mats * tiles,))],
            compiler_params=pltpu.CompilerParams(vmem_limit_bytes=2**20),
            name="write",
        )(x)

    spec = P(("rep", "dp"))
    return jax.shard_map(body, mesh=mesh, in_specs=(spec, spec), out_specs=P("rep"), check_vma=False)
```
